32 devices in a mesh: samp: 8 (over z, x), win: 1, snp: 4 (over y, core).
Axes of the slice: x: 2, y: 2, z: 4, core: 2. Of those that a mesh axis runs over, the one named last changes fastest.
Arguments:
- dosages: bfloat16 [4096, 4096], P('samp', ('win', 'snp')), may hold values from 0 to 2
Outputs:
- r_squared: float32 [1, 4096, 4096], P('win', 'samp', 'snp')
- band_r_squared: float32 [1, 1024, 4096], P('win', 'samp', 'snp')
The draws below stay inside these ranges and needn't reach their ends.
All inputs are finite; a program needn't handle non-finite values.
Results may differ from the reference program's by a relative error of at most 0.0003.
Values may be sent and summed in bfloat16 or wider, within the bound.
A program may use at most 128 MiB of HBM per device.

```python
import jax
import jax.numpy as jnp
from jax import lax

WS = 4096
OV = 1024
WINDOWS = 1
SAMPLES = 4096
SNPS = 4096


def draw_dosages(key, part):
    keys = jax.random.split(key, 5)
    span = min(24, SNPS)
    noise = jax.random.normal(keys[0], (SAMPLES, SNPS), jnp.float32)
    smooth = lax.reduce_window(noise, 0.0, lax.add, (1, span), (1, 1), 'SAME') / span ** 0.5
    own_weight = jax.random.uniform(keys[1], (SNPS,), jnp.float32, 0.3, 1.0)
    mix_weight = jax.random.uniform(keys[2], (SNPS,), jnp.float32, 0.5, 2.5)
    people = jax.random.normal(keys[3], (SAMPLES, 1), jnp.float32)
    loading = jax.random.normal(keys[4], (SNPS,), jnp.float32) * 0.6
    latent = noise * own_weight + smooth * mix_weight
    latent = latent + people * loading
    return (2.0 * jax.nn.sigmoid(latent)).astype(jnp.bfloat16)


def setup_inputs(seed: int = 0) -> dict:
    seeds = jax.random.split(jax.random.key(seed), 2)
    return {
        "dosages": draw_dosages(jax.random.fold_in(seeds[1], 71), 0),
    }


var_floor = 0.05


def squared_corr(gram, col_sum, col_sq, row_sum, row_sq, count):
    col_mean = col_sum / count
    row_mean = row_sum / count
    col_var = jnp.maximum(col_sq / count - col_mean * col_mean, var_floor)
    row_var = jnp.maximum(row_sq / count - row_mean * row_mean, var_floor)
    covar = gram / count - col_mean[:, None] * row_mean[None, :]
    return covar * covar / (col_var[:, None] * row_var[None, :])


def column_stats(block):
    wide = block.astype(jnp.float32)
    return jnp.sum(wide, axis=0), jnp.sum(wide * wide, axis=0)


def reference(dosages):
    count = jnp.float32(dosages.shape[0])
    whole_list = []
    band_list = []
    for window in range(WINDOWS):
        geno = dosages[:, window * WS:(window + 1) * WS]
        following = (window + 1) % WINDOWS
        after = dosages[:, following * WS:following * WS + OV]
        win_sum, win_sq = column_stats(geno)
        next_sum, next_sq = column_stats(after)
        gram = jnp.dot(geno.T, geno, preferred_element_type=jnp.float32)
        next_gram = jnp.dot(after.T, geno, preferred_element_type=jnp.float32)
        whole_list.append(squared_corr(gram, win_sum, win_sq, win_sum, win_sq, count))
        band_list.append(squared_corr(next_gram, next_sum, next_sq, win_sum, win_sq, count))
    return jnp.stack(whole_list), jnp.stack(band_list)
```

```python
import functools

import jax
import jax.numpy as jnp
from jax import lax
from jax.experimental import pallas as pl
from jax.experimental.pallas import tpu as pltpu
from jax.sharding import PartitionSpec as P

OV = 1024
VAR_FLOOR = 0.05
COLS = 2
PARTS = 2
MESH = pl.DeviceIdType.MESH


def plan(line):
    own = [(0, r, c) for r in range(line) for c in range(PARTS)]
    other = [(1, r, c) for r in range(line) for c in range(PARTS)]
    late = [v for v in other if v[1] in (1, 2) and v[2] == PARTS - 1]
    other = [v for v in other if v not in late] + late[::-1]
    lag = min(PARTS + 1, len(own))
    order = own[:lag]
    for k in range(lag, len(own)):
        order += [own[k], other[k - lag]]
    return order + other[len(own) - lag:]


def lookup(i, values):
    out = jnp.int32(0)
    for j, v in enumerate(values):
        if v:
            out = out + jnp.where(i == j, jnp.int32(v), jnp.int32(0))
    return out


def kernel(sizes, x_hbm, win_out, band_out, k_buf, j_buf, b_buf, k_stat, j_stat, b_stat,
           local_sem, k_recv, up_send, down_send, x_send, j_recv, j_send, b_recv, b_send, w_send, *band_wide):
    shard_count, windows, blocks, rows, width, jw, band, bw = sizes
    line = shard_count // COLS
    part_rows = rows // PARTS
    bits = blocks.bit_length() - 1
    chunks = shard_count * PARTS
    s = lax.axis_index("samp")
    n = lax.axis_index("snp")
    z = s // COLS
    x = s % COLS
    has_up = z < line - 1
    has_down = z > 0
    up = {"samp": jnp.minimum(s + COLS, shard_count - COLS + x)}
    down = {"samp": jnp.maximum(s - COLS, x)}
    across = {"samp": s + 1 - 2 * x}
    near = jnp.minimum(z, line - 1 - z)

    def bit(v, b):
        return (v // (1 << b)) % 2

    def flip(b):
        return {"snp": n + (1 << b) * (1 - 2 * bit(n, b))}

    j_home = (s * jw) // width
    j_off = pl.multiple_of((s * jw) % width, jw)
    b_home = (s * band) // width
    b_off = pl.multiple_of(((s * band) % width) // bw * bw, bw)
    j_rel = [(bit(n, b) + bit(j_home, b)) % 2 for b in range(bits)]
    b_rel = [(bit(n, b) + bit(b_home, b)) % 2 for b in range(bits)]

    def sends_on(rel, b):
        low = jnp.int32(0)
        for a in range(b + 1):
            low = low + rel[a]
        return low == 0

    def is_home(rel):
        total = jnp.int32(0)
        for r in rel:
            total = total + r
        return total == 0

    j_mine = is_home(j_rel)
    b_mine = is_home(b_rel)

    def k_copy(q, sem, to):
        return pltpu.make_async_remote_copy(
            src_ref=k_buf.at[q], dst_ref=k_buf.at[q], send_sem=sem.at[q], recv_sem=k_recv.at[q],
            device_id=to, device_id_type=MESH)

    def slice_copy(src, buf, q, send, recv, to):
        return pltpu.make_async_remote_copy(
            src_ref=src, dst_ref=buf.at[q], send_sem=send, recv_sem=recv.at[q],
            device_id=to, device_id_type=MESH)

    order = plan(line)
    band_sum = band_wide[0] if band_wide else band_out

    def item(o):
        side = lookup(o, [v[0] for v in order])
        r = lookup(o, [v[1] for v in order])
        c = lookup(o, [v[2] for v in order])
        odd = r % 2
        inner = z + jnp.where(odd == 1, 0 - (r + 1) // 2, r // 2)
        outer = jnp.where(z < line - 1 - z, r, line - 1 - r)
        zz = jnp.where(r <= 2 * near, inner, outer)
        xx = jnp.where(side == 1, 1 - x, x)
        return side, zz, c, (zz * COLS + xx) * PARTS + c

    def skips_x(zz, c):
        return (c == PARTS - 1) & ((zz == z + 1) | (zz == z - 1))

    for c in range(PARTS):
        pltpu.make_async_copy(x_hbm.at[pl.ds(c * part_rows, part_rows)],
                              k_buf.at[s * PARTS + c], local_sem.at[c]).start()

    barrier = pltpu.get_barrier_semaphore()

    def greet(to):
        pl.semaphore_signal(barrier, inc=1, device_id=to, device_id_type=MESH)

    pl.when(has_up)(lambda: greet(up))
    pl.when(has_down)(lambda: greet(down))
    greet(across)
    for b in range(bits):
        greet(flip(b))
    expected = 1 + bits
    if windows > 1:
        w = lax.axis_index("win")
        before = {"win": (w + windows - 1) % windows}
        after = {"win": (w + 1) % windows}
        greet(before)
        greet(after)
        expected += 2
    pl.semaphore_wait(barrier, expected + has_up.astype(jnp.int32) + has_down.astype(jnp.int32))

    k_stat[...] = jnp.zeros_like(k_stat)
    j_stat[...] = jnp.zeros_like(j_stat)
    b_stat[...] = jnp.zeros_like(b_stat)
    for c in range(PARTS):
        pltpu.make_async_copy(x_hbm.at[pl.ds(c * part_rows, part_rows)],
                              k_buf.at[s * PARTS + c], local_sem.at[c]).wait()

    last_own = max(i for i, v in enumerate(order) if v[0] == 0)
    cross_late = (s + 1 - 2 * x) * PARTS + PARTS - 1

    def take(o):
        side, zz, c, q = item(o)
        mine = (side == 0) & (zz == z)

        @pl.when(jnp.logical_not(mine))
        def _():
            k_copy(q, x_send, across).wait_recv()

        @pl.when((side == 0) & (zz <= z) & has_up)
        def _():
            k_copy(q, up_send, up).start()

        @pl.when((side == 0) & (zz >= z) & has_down)
        def _():
            k_copy(q, down_send, down).start()

        @pl.when((side == 0) & jnp.logical_not(skips_x(zz, c)))
        def _():
            k_copy(q, x_send, across).start()

        if line > 1:
            @pl.when((o == last_own) & has_up)
            def _():
                k_copy(cross_late, up_send, up).start()

            @pl.when((o == last_own) & has_down)
            def _():
                k_copy(cross_late, down_send, down).start()

        for b in reversed(range(bits)):
            @pl.when(j_mine)
            def _():
                slice_copy(k_buf.at[q, :, pl.ds(j_off, jw)], j_buf, q, j_send.at[b, q], j_recv, flip(b)).start()

            if windows == 1:
                @pl.when(b_mine)
                def _():
                    slice_copy(k_buf.at[q, :, pl.ds(b_off, bw)], b_buf, q, b_send.at[b, q], b_recv, flip(b)).start()
        if windows > 1:
            @pl.when(b_mine)
            def _():
                slice_copy(k_buf.at[q, :, pl.ds(b_off, bw)], b_buf, q, w_send.at[q], b_recv, before).start()

    def j_arrive(q):
        slice_copy(k_buf.at[q, :, pl.ds(j_off, jw)], j_buf, q, j_send.at[0, q], j_recv, flip(0)).wait_recv()

    def b_arrive(q):
        slice_copy(k_buf.at[q, :, pl.ds(b_off, bw)], b_buf, q, b_send.at[0, q], b_recv, flip(0)).wait_recv()

    def relay(o):
        _, _, _, q = item(o)

        @pl.when(jnp.logical_not(j_mine))
        def _():
            j_arrive(q)
            for b in reversed(range(bits)):
                @pl.when(sends_on(j_rel, b))
                def _():
                    slice_copy(j_buf.at[q], j_buf, q, j_send.at[b, q], j_recv, flip(b)).start()

        @pl.when(j_mine)
        def _():
            j_buf[q] = k_buf[q, :, pl.ds(j_off, jw)]

        def pass_band():
            b_arrive(q)
            for b in reversed(range(bits)):
                @pl.when(sends_on(b_rel, b))
                def _():
                    slice_copy(b_buf.at[q], b_buf, q, b_send.at[b, q], b_recv, flip(b)).start()

        if windows > 1:
            pass_band()
        else:
            pl.when(jnp.logical_not(b_mine))(pass_band)

            @pl.when(b_mine)
            def _():
                b_buf[q] = k_buf[q, :, pl.ds(b_off, bw)]

    def add_stats(stat, block):
        wide = block.astype(jnp.float32).reshape(part_rows // 8, 8, block.shape[-1])
        stat[0] += jnp.sum(wide, axis=0)
        stat[1] += jnp.sum(wide * wide, axis=0)

    def pair(a, b):
        return lax.dot_general(a, b, (((0,), (0,)), ((), ())), preferred_element_type=jnp.float32)

    def compute(o):
        _, _, _, q = item(o)
        whole = k_buf[q]
        j_cols = j_buf[q]
        b_cols = b_buf[q]
        add_stats(k_stat, whole)
        add_stats(j_stat, j_cols)
        add_stats(b_stat, b_cols)

        @pl.when(o == 0)
        def _():
            win_out[0] = pair(j_cols, whole)
            band_sum[0] = pair(b_cols, whole)

        @pl.when(o > 0)
        def _():
            win_out[0] += pair(j_cols, whole)
            band_sum[0] += pair(b_cols, whole)

    def step(o, carry):
        @pl.when(o < chunks)
        def _():
            take(o)

        @pl.when((o >= 1) & (o < chunks + 1))
        def _():
            relay(o - 1)

        @pl.when(o >= 2)
        def _():
            compute(o - 2)

        return carry

    lax.fori_loop(0, chunks + 2, step, 0)

    count = jnp.float32(rows * shard_count)

    def moments(total, square):
        mean = total / count
        return mean, 1.0 / jnp.maximum(square / count - mean * mean, VAR_FLOOR)

    row_mean, row_inv = moments(jnp.sum(k_stat[0], axis=0, keepdims=True), jnp.sum(k_stat[1], axis=0, keepdims=True))

    def finish(out, stat, height):
        mean, inv = moments(jnp.sum(stat[0].T, axis=1, keepdims=True), jnp.sum(stat[1].T, axis=1, keepdims=True))
        for a in range(0, height, 64):
            e = min(a + 64, height)
            covar = out[0, a:e] / count - mean[a:e] * row_mean
            out[0, a:e] = covar * covar * (inv[a:e] * row_inv)

    finish(win_out, j_stat, jw)
    finish(band_sum, b_stat, bw)
    if band_wide:
        band_out[0] = band_sum[0, pl.ds(pl.multiple_of((s * band) % bw, band), band)]

    def drain(o, carry):
        side, zz, c, q = item(o)

        @pl.when((side == 0) & (zz <= z) & has_up)
        def _():
            k_copy(q, up_send, up).wait_send()

        @pl.when((side == 0) & (zz >= z) & has_down)
        def _():
            k_copy(q, down_send, down).wait_send()

        @pl.when((side == 0) & jnp.logical_not(skips_x(zz, c)))
        def _():
            k_copy(q, x_send, across).wait_send()

        for b in range(bits):
            @pl.when(sends_on(j_rel, b))
            def _():
                slice_copy(j_buf.at[q], j_buf, q, j_send.at[b, q], j_recv, flip(b)).wait_send()

            @pl.when(sends_on(b_rel, b))
            def _():
                slice_copy(b_buf.at[q], b_buf, q, b_send.at[b, q], b_recv, flip(b)).wait_send()
        if windows > 1:
            @pl.when(b_mine)
            def _():
                slice_copy(b_buf.at[q], b_buf, q, w_send.at[q], b_recv, before).wait_send()
        return carry

    lax.fori_loop(0, chunks, drain, 0)
    if line > 1:
        @pl.when(has_up)
        def _():
            k_copy(cross_late, up_send, up).wait_send()

        @pl.when(has_down)
        def _():
            k_copy(cross_late, down_send, down).wait_send()


def shards(dosages):
    rows, width = dosages.shape
    shard_count = lax.axis_size("samp")
    windows = lax.axis_size("win")
    blocks = lax.axis_size("snp")
    jw = width * blocks // shard_count
    band = OV // shard_count
    bw = max(band, 128)
    bits = blocks.bit_length() - 1
    chunks = shard_count * PARTS
    part_rows = rows // PARTS
    sizes = (shard_count, windows, blocks, rows, width, jw, band, bw)
    dma = pltpu.SemaphoreType.DMA
    return pl.pallas_call(
        functools.partial(kernel, sizes),
        out_shape=(
            jax.ShapeDtypeStruct((1, jw, width), jnp.float32),
            jax.ShapeDtypeStruct((1, band, width), jnp.float32),
        ),
        in_specs=[pl.BlockSpec(memory_space=pl.ANY)],
        out_specs=[pl.BlockSpec(memory_space=pltpu.VMEM)] * 2,
        scratch_shapes=[
            pltpu.VMEM((chunks, part_rows, width), jnp.bfloat16),
            pltpu.VMEM((chunks, part_rows, jw), jnp.bfloat16),
            pltpu.VMEM((chunks, part_rows, bw), jnp.bfloat16),
            pltpu.VMEM((2, 8, width), jnp.float32),
            pltpu.VMEM((2, 8, jw), jnp.float32),
            pltpu.VMEM((2, 8, bw), jnp.float32),
            dma((PARTS,)),
            dma((chunks,)), dma((chunks,)), dma((chunks,)), dma((chunks,)),
            dma((chunks,)), dma((bits, chunks)),
            dma((chunks,)), dma((bits, chunks)), dma((chunks,)),
        ] + ([pltpu.VMEM((1, bw, width), jnp.float32)] if bw != band else []),
        compiler_params=pltpu.CompilerParams(
            collective_id=0, has_side_effects=True, vmem_limit_bytes=67043328
        ),
    )(dosages)


def solution(mesh):
    return jax.shard_map(
        shards,
        mesh=mesh,
        in_specs=(P("samp", ("win", "snp")),),
        out_specs=(P("win", "samp", "snp"), P("win", "samp", "snp")),
        check_vma=False,
    )
```

```python
import functools

import jax
import jax.numpy as jnp
from jax import lax
from jax.experimental import pallas as pl
from jax.experimental.pallas import tpu as pltpu
from jax.sharding import PartitionSpec as P

OV = 1024
VAR_FLOOR = 0.05
COLS = 2
PARTS = 4
LATE = PARTS // 2
MESH = pl.DeviceIdType.MESH


def plan(line):
    own = [(0, r, c) for r in range(line) for c in range(PARTS)]
    other = [(1, r, c) for r in range(line) for c in range(PARTS)]
    late = [v for v in other if v[1] in (1, 2) and v[2] >= LATE]
    other = [v for v in other if v not in late]
    other = other[:-1] + [v for v in late if v[1] == 2] + other[-1:] + [v for v in late if v[1] == 1]
    lag = min(PARTS + 1, len(own))
    order = own[:lag]
    for k in range(lag, len(own)):
        order += [own[k], other[k - lag]]
    return order + other[len(own) - lag:]


def lookup(i, values):
    out = jnp.int32(0)
    for j, v in enumerate(values):
        if v:
            out = out + jnp.where(i == j, jnp.int32(v), jnp.int32(0))
    return out


def kernel(sizes, x_hbm, win_out, band_out, k_buf, j_buf, b_buf, k_stat, j_stat, b_stat,
           local_sem, k_recv, up_send, down_send, x_send, j_recv, j_send, b_recv, b_send, w_send, *band_wide):
    shard_count, windows, blocks, rows, width, jw, band, bw = sizes
    line = shard_count // COLS
    part_rows = rows // PARTS
    bits = blocks.bit_length() - 1
    chunks = shard_count * PARTS
    s = lax.axis_index("samp")
    n = lax.axis_index("snp")
    z = s // COLS
    x = s % COLS
    has_up = z < line - 1
    has_down = z > 0
    up = {"samp": jnp.minimum(s + COLS, shard_count - COLS + x)}
    down = {"samp": jnp.maximum(s - COLS, x)}
    across = {"samp": s + 1 - 2 * x}
    near = jnp.minimum(z, line - 1 - z)

    def bit(v, b):
        return (v // (1 << b)) % 2

    def flip(b):
        return {"snp": n + (1 << b) * (1 - 2 * bit(n, b))}

    j_home = (s * jw) // width
    j_off = pl.multiple_of((s * jw) % width, jw)
    b_home = (s * band) // width
    b_off = pl.multiple_of(((s * band) % width) // bw * bw, bw)
    j_rel = [(bit(n, b) + bit(j_home, b)) % 2 for b in range(bits)]
    b_rel = [(bit(n, b) + bit(b_home, b)) % 2 for b in range(bits)]

    def sends_on(rel, b):
        low = jnp.int32(0)
        for a in range(b + 1):
            low = low + rel[a]
        return low == 0

    def is_home(rel):
        total = jnp.int32(0)
        for r in rel:
            total = total + r
        return total == 0

    j_mine = is_home(j_rel)
    b_mine = is_home(b_rel)

    def k_copy(q, sem, to):
        return pltpu.make_async_remote_copy(
            src_ref=k_buf.at[q], dst_ref=k_buf.at[q], send_sem=sem.at[q], recv_sem=k_recv.at[q],
            device_id=to, device_id_type=MESH)

    def slice_copy(src, buf, q, send, recv, to):
        return pltpu.make_async_remote_copy(
            src_ref=src, dst_ref=buf.at[q], send_sem=send, recv_sem=recv.at[q],
            device_id=to, device_id_type=MESH)

    order = plan(line)
    band_sum = band_wide[0] if band_wide else band_out

    def item(o):
        side = lookup(o, [v[0] for v in order])
        r = lookup(o, [v[1] for v in order])
        c = lookup(o, [v[2] for v in order])
        odd = r % 2
        inner = z + jnp.where(odd == 1, 0 - (r + 1) // 2, r // 2)
        outer = jnp.where(z < line - 1 - z, r, line - 1 - r)
        zz = jnp.where(r <= 2 * near, inner, outer)
        xx = jnp.where(side == 1, 1 - x, x)
        return side, zz, c, (zz * COLS + xx) * PARTS + c

    def skips_x(zz, c):
        return (c >= LATE) & ((zz == z + 1) | (zz == z - 1))

    for c in range(PARTS):
        pltpu.make_async_copy(x_hbm.at[pl.ds(c * part_rows, part_rows)],
                              k_buf.at[s * PARTS + c], local_sem.at[c]).start()

    barrier = pltpu.get_barrier_semaphore()

    def greet(to):
        pl.semaphore_signal(barrier, inc=1, device_id=to, device_id_type=MESH)

    pl.when(has_up)(lambda: greet(up))
    pl.when(has_down)(lambda: greet(down))
    greet(across)
    for b in range(bits):
        greet(flip(b))
    expected = 1 + bits
    if windows > 1:
        w = lax.axis_index("win")
        before = {"win": (w + windows - 1) % windows}
        after = {"win": (w + 1) % windows}
        greet(before)
        greet(after)
        expected += 2
    pl.semaphore_wait(barrier, expected + has_up.astype(jnp.int32) + has_down.astype(jnp.int32))

    k_stat[...] = jnp.zeros_like(k_stat)
    j_stat[...] = jnp.zeros_like(j_stat)
    b_stat[...] = jnp.zeros_like(b_stat)
    for c in range(PARTS):
        pltpu.make_async_copy(x_hbm.at[pl.ds(c * part_rows, part_rows)],
                              k_buf.at[s * PARTS + c], local_sem.at[c]).wait()

    last_own = max(i for i, v in enumerate(order) if v[0] == 0)
    cross_late = [(s + 1 - 2 * x) * PARTS + c for c in range(LATE, PARTS)]

    def take(o):
        side, zz, c, q = item(o)
        mine = (side == 0) & (zz == z)

        @pl.when(jnp.logical_not(mine))
        def _():
            k_copy(q, x_send, across).wait_recv()

        @pl.when((side == 0) & (zz <= z) & has_up)
        def _():
            k_copy(q, up_send, up).start()

        @pl.when((side == 0) & (zz >= z) & has_down)
        def _():
            k_copy(q, down_send, down).start()

        @pl.when((side == 0) & jnp.logical_not(skips_x(zz, c)))
        def _():
            k_copy(q, x_send, across).start()

        if line > 1:
            @pl.when((o == last_own) & has_up)
            def _():
                for late in cross_late:
                    k_copy(late, up_send, up).start()

            @pl.when((o == last_own) & has_down)
            def _():
                for late in cross_late:
                    k_copy(late, down_send, down).start()

        for b in reversed(range(bits)):
            @pl.when(j_mine)
            def _():
                slice_copy(k_buf.at[q, :, pl.ds(j_off, jw)], j_buf, q, j_send.at[b, q], j_recv, flip(b)).start()

            if windows == 1:
                @pl.when(b_mine)
                def _():
                    slice_copy(k_buf.at[q, :, pl.ds(b_off, bw)], b_buf, q, b_send.at[b, q], b_recv, flip(b)).start()
        if windows > 1:
            @pl.when(b_mine)
            def _():
                slice_copy(k_buf.at[q, :, pl.ds(b_off, bw)], b_buf, q, w_send.at[q], b_recv, before).start()

    def j_arrive(q):
        slice_copy(k_buf.at[q, :, pl.ds(j_off, jw)], j_buf, q, j_send.at[0, q], j_recv, flip(0)).wait_recv()

    def b_arrive(q):
        slice_copy(k_buf.at[q, :, pl.ds(b_off, bw)], b_buf, q, b_send.at[0, q], b_recv, flip(0)).wait_recv()

    def relay(o):
        _, _, _, q = item(o)

        @pl.when(jnp.logical_not(j_mine))
        def _():
            j_arrive(q)
            for b in reversed(range(bits)):
                @pl.when(sends_on(j_rel, b))
                def _():
                    slice_copy(j_buf.at[q], j_buf, q, j_send.at[b, q], j_recv, flip(b)).start()

        @pl.when(j_mine)
        def _():
            j_buf[q] = k_buf[q, :, pl.ds(j_off, jw)]

        def pass_band():
            b_arrive(q)
            for b in reversed(range(bits)):
                @pl.when(sends_on(b_rel, b))
                def _():
                    slice_copy(b_buf.at[q], b_buf, q, b_send.at[b, q], b_recv, flip(b)).start()

        if windows > 1:
            pass_band()
        else:
            pl.when(jnp.logical_not(b_mine))(pass_band)

            @pl.when(b_mine)
            def _():
                b_buf[q] = k_buf[q, :, pl.ds(b_off, bw)]

    def add_stats(stat, block):
        wide = block.astype(jnp.float32).reshape(part_rows // 8, 8, block.shape[-1])
        stat[0] += jnp.sum(wide, axis=0)
        stat[1] += jnp.sum(wide * wide, axis=0)

    def pair(a, b):
        return lax.dot_general(a, b, (((0,), (0,)), ((), ())), preferred_element_type=jnp.float32)

    def compute(o):
        _, _, _, q = item(o)
        whole = k_buf[q]
        j_cols = j_buf[q]
        b_cols = b_buf[q]
        add_stats(k_stat, whole)
        add_stats(j_stat, j_cols)
        add_stats(b_stat, b_cols)

        @pl.when(o == 0)
        def _():
            win_out[0] = pair(j_cols, whole)
            band_sum[0] = pair(b_cols, whole)

        @pl.when(o > 0)
        def _():
            win_out[0] += pair(j_cols, whole)
            band_sum[0] += pair(b_cols, whole)

    def step(o, carry):
        @pl.when(o < chunks)
        def _():
            take(o)

        @pl.when((o >= 2) & (o < chunks + 2))
        def _():
            relay(o - 2)

        @pl.when(o >= 3)
        def _():
            compute(o - 3)

        return carry

    lax.fori_loop(0, chunks + 3, step, 0)

    count = jnp.float32(rows * shard_count)

    def moments(total, square):
        mean = total / count
        return mean, 1.0 / jnp.maximum(square / count - mean * mean, VAR_FLOOR)

    row_mean, row_inv = moments(jnp.sum(k_stat[0], axis=0, keepdims=True), jnp.sum(k_stat[1], axis=0, keepdims=True))

    def finish(out, stat, height):
        mean, inv = moments(jnp.sum(stat[0].T, axis=1, keepdims=True), jnp.sum(stat[1].T, axis=1, keepdims=True))
        for a in range(0, height, 64):
            e = min(a + 64, height)
            covar = out[0, a:e] / count - mean[a:e] * row_mean
            out[0, a:e] = covar * covar * (inv[a:e] * row_inv)

    finish(win_out, j_stat, jw)
    finish(band_sum, b_stat, bw)
    if band_wide:
        band_out[0] = band_sum[0, pl.ds(pl.multiple_of((s * band) % bw, band), band)]

    def drain(o, carry):
        side, zz, c, q = item(o)

        @pl.when((side == 0) & (zz <= z) & has_up)
        def _():
            k_copy(q, up_send, up).wait_send()

        @pl.when((side == 0) & (zz >= z) & has_down)
        def _():
            k_copy(q, down_send, down).wait_send()

        @pl.when((side == 0) & jnp.logical_not(skips_x(zz, c)))
        def _():
            k_copy(q, x_send, across).wait_send()

        for b in range(bits):
            @pl.when(sends_on(j_rel, b))
            def _():
                slice_copy(j_buf.at[q], j_buf, q, j_send.at[b, q], j_recv, flip(b)).wait_send()

            @pl.when(sends_on(b_rel, b))
            def _():
                slice_copy(b_buf.at[q], b_buf, q, b_send.at[b, q], b_recv, flip(b)).wait_send()
        if windows > 1:
            @pl.when(b_mine)
            def _():
                slice_copy(b_buf.at[q], b_buf, q, w_send.at[q], b_recv, before).wait_send()
        return carry

    lax.fori_loop(0, chunks, drain, 0)
    if line > 1:
        @pl.when(has_up)
        def _():
            for late in cross_late:
                k_copy(late, up_send, up).wait_send()

        @pl.when(has_down)
        def _():
            for late in cross_late:
                k_copy(late, down_send, down).wait_send()


def shards(dosages):
    rows, width = dosages.shape
    shard_count = lax.axis_size("samp")
    windows = lax.axis_size("win")
    blocks = lax.axis_size("snp")
    jw = width * blocks // shard_count
    band = OV // shard_count
    bw = max(band, 128)
    bits = blocks.bit_length() - 1
    chunks = shard_count * PARTS
    part_rows = rows // PARTS
    sizes = (shard_count, windows, blocks, rows, width, jw, band, bw)
    dma = pltpu.SemaphoreType.DMA
    return pl.pallas_call(
        functools.partial(kernel, sizes),
        out_shape=(
            jax.ShapeDtypeStruct((1, jw, width), jnp.float32),
            jax.ShapeDtypeStruct((1, band, width), jnp.float32),
        ),
        in_specs=[pl.BlockSpec(memory_space=pl.ANY)],
        out_specs=[pl.BlockSpec(memory_space=pltpu.VMEM)] * 2,
        scratch_shapes=[
            pltpu.VMEM((chunks, part_rows, width), jnp.bfloat16),
            pltpu.VMEM((chunks, part_rows, jw), jnp.bfloat16),
            pltpu.VMEM((chunks, part_rows, bw), jnp.bfloat16),
            pltpu.VMEM((2, 8, width), jnp.float32),
            pltpu.VMEM((2, 8, jw), jnp.float32),
            pltpu.VMEM((2, 8, bw), jnp.float32),
            dma((PARTS,)),
            dma((chunks,)), dma((chunks,)), dma((chunks,)), dma((chunks,)),
            dma((chunks,)), dma((bits, chunks)),
            dma((chunks,)), dma((bits, chunks)), dma((chunks,)),
        ] + ([pltpu.VMEM((1, bw, width), jnp.float32)] if bw != band else []),
        compiler_params=pltpu.CompilerParams(
            collective_id=0, has_side_effects=True, vmem_limit_bytes=67043328
        ),
    )(dosages)


def solution(mesh):
    return jax.shard_map(
        shards,
        mesh=mesh,
        in_specs=(P("samp", ("win", "snp")),),
        out_specs=(P("win", "samp", "snp"), P("win", "samp", "snp")),
        check_vma=False,
    )
```

```python
import functools

import jax
import jax.numpy as jnp
from jax import lax
from jax.experimental import pallas as pl
from jax.experimental.pallas import tpu as pltpu
from jax.sharding import PartitionSpec as P

OV = 1024
VAR_FLOOR = 0.05
COLS = 2
PARTS = 2
MESH = pl.DeviceIdType.MESH


def plan(line):
    own = [(0, r, c) for r in range(line) for c in range(PARTS)]
    other = [(1, r, c) for r in range(line) for c in range(PARTS)]
    late = [v for v in other if v[1] in (1, 2) and v[2] == PARTS - 1]
    other = [v for v in other if v not in late] + late[::-1]
    lag = min(PARTS + 1, len(own))
    order = own[:lag]
    for k in range(lag, len(own)):
        order += [own[k], other[k - lag]]
    return order + other[len(own) - lag:]


def lookup(i, values):
    out = jnp.int32(0)
    for j, v in enumerate(values):
        if v:
            out = out + jnp.where(i == j, jnp.int32(v), jnp.int32(0))
    return out


def kernel(sizes, x_hbm, win_out, band_out, k_buf, j_buf, b_buf, k_stat, j_stat, b_stat,
           local_sem, k_recv, up_send, down_send, x_send, j_recv, j_send, b_recv, b_send, w_send, *band_wide):
    shard_count, windows, blocks, rows, width, jw, band, bw = sizes
    line = shard_count // COLS
    part_rows = rows // PARTS
    bits = blocks.bit_length() - 1
    chunks = shard_count * PARTS
    s = lax.axis_index("samp")
    n = lax.axis_index("snp")
    z = s // COLS
    x = s % COLS
    has_up = z < line - 1
    has_down = z > 0
    up = {"samp": jnp.minimum(s + COLS, shard_count - COLS + x)}
    down = {"samp": jnp.maximum(s - COLS, x)}
    across = {"samp": s + 1 - 2 * x}
    near = jnp.minimum(z, line - 1 - z)

    def bit(v, b):
        return (v // (1 << b)) % 2

    def flip(b):
        return {"snp": n + (1 << b) * (1 - 2 * bit(n, b))}

    j_home = (s * jw) // width
    j_off = pl.multiple_of((s * jw) % width, jw)
    b_home = (s * band) // width
    b_off = pl.multiple_of(((s * band) % width) // bw * bw, bw)
    j_rel = [(bit(n, b) + bit(j_home, b)) % 2 for b in range(bits)]
    b_rel = [(bit(n, b) + bit(b_home, b)) % 2 for b in range(bits)]

    def sends_on(rel, b):
        low = jnp.int32(0)
        for a in range(b + 1):
            low = low + rel[a]
        return low == 0

    def is_home(rel):
        total = jnp.int32(0)
        for r in rel:
            total = total + r
        return total == 0

    j_mine = is_home(j_rel)
    b_mine = is_home(b_rel)

    def k_copy(q, sem, to):
        return pltpu.make_async_remote_copy(
            src_ref=k_buf.at[q], dst_ref=k_buf.at[q], send_sem=sem.at[q], recv_sem=k_recv.at[q],
            device_id=to, device_id_type=MESH)

    def slice_copy(src, buf, q, send, recv, to):
        return pltpu.make_async_remote_copy(
            src_ref=src, dst_ref=buf.at[q], send_sem=send, recv_sem=recv.at[q],
            device_id=to, device_id_type=MESH)

    order = plan(line)
    band_sum = band_wide[0] if band_wide else band_out

    def item(o):
        side = lookup(o, [v[0] for v in order])
        r = lookup(o, [v[1] for v in order])
        c = lookup(o, [v[2] for v in order])
        odd = r % 2
        inner = z + jnp.where(odd == 1, 0 - (r + 1) // 2, r // 2)
        outer = jnp.where(z < line - 1 - z, r, line - 1 - r)
        zz = jnp.where(r <= 2 * near, inner, outer)
        xx = jnp.where(side == 1, 1 - x, x)
        return side, zz, c, (zz * COLS + xx) * PARTS + c

    def skips_x(zz, c):
        return (c == PARTS - 1) & ((zz == z + 1) | (zz == z - 1))

    for c in range(PARTS):
        pltpu.make_async_copy(x_hbm.at[pl.ds(c * part_rows, part_rows)],
                              k_buf.at[s * PARTS + c], local_sem.at[c]).start()

    barrier = pltpu.get_barrier_semaphore()

    def greet(to):
        pl.semaphore_signal(barrier, inc=1, device_id=to, device_id_type=MESH)

    pl.when(has_up)(lambda: greet(up))
    pl.when(has_down)(lambda: greet(down))
    greet(across)
    for b in range(bits):
        greet(flip(b))
    expected = 1 + bits
    if windows > 1:
        w = lax.axis_index("win")
        before = {"win": (w + windows - 1) % windows}
        after = {"win": (w + 1) % windows}
        greet(before)
        greet(after)
        expected += 2
    pl.semaphore_wait(barrier, expected + has_up.astype(jnp.int32) + has_down.astype(jnp.int32))

    k_stat[...] = jnp.zeros_like(k_stat)
    j_stat[...] = jnp.zeros_like(j_stat)
    b_stat[...] = jnp.zeros_like(b_stat)
    for c in range(PARTS):
        pltpu.make_async_copy(x_hbm.at[pl.ds(c * part_rows, part_rows)],
                              k_buf.at[s * PARTS + c], local_sem.at[c]).wait()

    last_own = max(i for i, v in enumerate(order) if v[0] == 0)
    cross_late = (s + 1 - 2 * x) * PARTS + PARTS - 1

    def take(o):
        side, zz, c, q = item(o)
        mine = (side == 0) & (zz == z)

        @pl.when(jnp.logical_not(mine))
        def _():
            k_copy(q, x_send, across).wait_recv()

        @pl.when((side == 0) & (zz <= z) & has_up)
        def _():
            k_copy(q, up_send, up).start()

        @pl.when((side == 0) & (zz >= z) & has_down)
        def _():
            k_copy(q, down_send, down).start()

        @pl.when((side == 0) & jnp.logical_not(skips_x(zz, c)))
        def _():
            k_copy(q, x_send, across).start()

        if line > 1:
            @pl.when((o == last_own) & has_up)
            def _():
                k_copy(cross_late, up_send, up).start()

            @pl.when((o == last_own) & has_down)
            def _():
                k_copy(cross_late, down_send, down).start()

        for b in reversed(range(bits)):
            @pl.when(j_mine)
            def _():
                slice_copy(k_buf.at[q, :, pl.ds(j_off, jw)], j_buf, q, j_send.at[b, q], j_recv, flip(b)).start()

            if windows == 1:
                @pl.when(b_mine)
                def _():
                    slice_copy(k_buf.at[q, :, pl.ds(b_off, bw)], b_buf, q, b_send.at[b, q], b_recv, flip(b)).start()
        if windows > 1:
            @pl.when(b_mine)
            def _():
                slice_copy(k_buf.at[q, :, pl.ds(b_off, bw)], b_buf, q, w_send.at[q], b_recv, before).start()

    def j_arrive(q):
        slice_copy(k_buf.at[q, :, pl.ds(j_off, jw)], j_buf, q, j_send.at[0, q], j_recv, flip(0)).wait_recv()

    def b_arrive(q):
        slice_copy(k_buf.at[q, :, pl.ds(b_off, bw)], b_buf, q, b_send.at[0, q], b_recv, flip(0)).wait_recv()

    def relay(o):
        _, _, _, q = item(o)

        @pl.when(jnp.logical_not(j_mine))
        def _():
            j_arrive(q)
            for b in reversed(range(bits)):
                @pl.when(sends_on(j_rel, b))
                def _():
                    slice_copy(j_buf.at[q], j_buf, q, j_send.at[b, q], j_recv, flip(b)).start()

        @pl.when(j_mine)
        def _():
            j_buf[q] = k_buf[q, :, pl.ds(j_off, jw)]

        def pass_band():
            b_arrive(q)
            for b in reversed(range(bits)):
                @pl.when(sends_on(b_rel, b))
                def _():
                    slice_copy(b_buf.at[q], b_buf, q, b_send.at[b, q], b_recv, flip(b)).start()

        if windows > 1:
            pass_band()
        else:
            pl.when(jnp.logical_not(b_mine))(pass_band)

            @pl.when(b_mine)
            def _():
                b_buf[q] = k_buf[q, :, pl.ds(b_off, bw)]

    def add_stats(stat, block):
        wide = block.astype(jnp.float32).reshape(part_rows // 8, 8, block.shape[-1])
        stat[0] += jnp.sum(wide, axis=0)
        stat[1] += jnp.sum(wide * wide, axis=0)

    def pair(a, b):
        return lax.dot_general(a, b, (((0,), (0,)), ((), ())), preferred_element_type=jnp.float32)

    def compute(o):
        _, _, _, q = item(o)
        whole = k_buf[q]
        j_cols = j_buf[q]
        b_cols = b_buf[q]
        add_stats(k_stat, whole)
        add_stats(j_stat, j_cols)
        add_stats(b_stat, b_cols)

        @pl.when(o == 0)
        def _():
            win_out[0] = pair(j_cols, whole)
            band_sum[0] = pair(b_cols, whole)

        @pl.when(o > 0)
        def _():
            win_out[0] += pair(j_cols, whole)
            band_sum[0] += pair(b_cols, whole)

    def step(o, carry):
        @pl.when(o < chunks)
        def _():
            take(o)

        @pl.when((o >= 2) & (o < chunks + 2))
        def _():
            relay(o - 2)

        @pl.when(o >= 3)
        def _():
            compute(o - 3)

        return carry

    lax.fori_loop(0, chunks + 3, step, 0)

    count = jnp.float32(rows * shard_count)

    def moments(total, square):
        mean = total / count
        return mean, 1.0 / jnp.maximum(square / count - mean * mean, VAR_FLOOR)

    row_mean, row_inv = moments(jnp.sum(k_stat[0], axis=0, keepdims=True), jnp.sum(k_stat[1], axis=0, keepdims=True))

    def finish(out, stat, height):
        mean, inv = moments(jnp.sum(stat[0].T, axis=1, keepdims=True), jnp.sum(stat[1].T, axis=1, keepdims=True))
        for a in range(0, height, 64):
            e = min(a + 64, height)
            covar = out[0, a:e] / count - mean[a:e] * row_mean
            out[0, a:e] = covar * covar * (inv[a:e] * row_inv)

    finish(win_out, j_stat, jw)
    finish(band_sum, b_stat, bw)
    if band_wide:
        band_out[0] = band_sum[0, pl.ds(pl.multiple_of((s * band) % bw, band), band)]

    def drain(o, carry):
        side, zz, c, q = item(o)

        @pl.when((side == 0) & (zz <= z) & has_up)
        def _():
            k_copy(q, up_send, up).wait_send()

        @pl.when((side == 0) & (zz >= z) & has_down)
        def _():
            k_copy(q, down_send, down).wait_send()

        @pl.when((side == 0) & jnp.logical_not(skips_x(zz, c)))
        def _():
            k_copy(q, x_send, across).wait_send()

        for b in range(bits):
            @pl.when(sends_on(j_rel, b))
            def _():
                slice_copy(j_buf.at[q], j_buf, q, j_send.at[b, q], j_recv, flip(b)).wait_send()

            @pl.when(sends_on(b_rel, b))
            def _():
                slice_copy(b_buf.at[q], b_buf, q, b_send.at[b, q], b_recv, flip(b)).wait_send()
        if windows > 1:
            @pl.when(b_mine)
            def _():
                slice_copy(b_buf.at[q], b_buf, q, w_send.at[q], b_recv, before).wait_send()
        return carry

    lax.fori_loop(0, chunks, drain, 0)
    if line > 1:
        @pl.when(has_up)
        def _():
            k_copy(cross_late, up_send, up).wait_send()

        @pl.when(has_down)
        def _():
            k_copy(cross_late, down_send, down).wait_send()


def shards(dosages):
    rows, width = dosages.shape
    shard_count = lax.axis_size("samp")
    windows = lax.axis_size("win")
    blocks = lax.axis_size("snp")
    jw = width * blocks // shard_count
    band = OV // shard_count
    bw = max(band, 128)
    bits = blocks.bit_length() - 1
    chunks = shard_count * PARTS
    part_rows = rows // PARTS
    sizes = (shard_count, windows, blocks, rows, width, jw, band, bw)
    dma = pltpu.SemaphoreType.DMA
    return pl.pallas_call(
        functools.partial(kernel, sizes),
        out_shape=(
            jax.ShapeDtypeStruct((1, jw, width), jnp.float32),
            jax.ShapeDtypeStruct((1, band, width), jnp.float32),
        ),
        in_specs=[pl.BlockSpec(memory_space=pl.ANY)],
        out_specs=[pl.BlockSpec(memory_space=pltpu.VMEM)] * 2,
        scratch_shapes=[
            pltpu.VMEM((chunks, part_rows, width), jnp.bfloat16),
            pltpu.VMEM((chunks, part_rows, jw), jnp.bfloat16),
            pltpu.VMEM((chunks, part_rows, bw), jnp.bfloat16),
            pltpu.VMEM((2, 8, width), jnp.float32),
            pltpu.VMEM((2, 8, jw), jnp.float32),
            pltpu.VMEM((2, 8, bw), jnp.float32),
            dma((PARTS,)),
            dma((chunks,)), dma((chunks,)), dma((chunks,)), dma((chunks,)),
            dma((chunks,)), dma((bits, chunks)),
            dma((chunks,)), dma((bits, chunks)), dma((chunks,)),
        ] + ([pltpu.VMEM((1, bw, width), jnp.float32)] if bw != band else []),
        compiler_params=pltpu.CompilerParams(
            collective_id=0, has_side_effects=True, vmem_limit_bytes=67043328
        ),
    )(dosages)


def solution(mesh):
    return jax.shard_map(
        shards,
        mesh=mesh,
        in_specs=(P("samp", ("win", "snp")),),
        out_specs=(P("win", "samp", "snp"), P("win", "samp", "snp")),
        check_vma=False,
    )
```

```python
import functools

import jax
import jax.numpy as jnp
from jax import lax
from jax.experimental import pallas as pl
from jax.experimental.pallas import tpu as pltpu
from jax.sharding import PartitionSpec as P

OV = 1024
VAR_FLOOR = 0.05
COLS = 2
PARTS = 2
MESH = pl.DeviceIdType.MESH


def plan(line):
    own = [(0, r, c) for r in range(line) for c in range(PARTS)]
    other = [(1, r, c) for r in range(line) for c in range(PARTS)]
    late = [v for v in other if v[1] in (1, 2) and v[2] == PARTS - 1]
    other = [v for v in other if v not in late]
    other = other[:-1] + [v for v in late if v[1] == 2] + other[-1:] + [v for v in late if v[1] == 1]
    lag = min(PARTS + 1, len(own))
    order = own[:lag]
    for k in range(lag, len(own)):
        order += [own[k], other[k - lag]]
    return order + other[len(own) - lag:]


def lookup(i, values):
    out = jnp.int32(0)
    for j, v in enumerate(values):
        if v:
            out = out + jnp.where(i == j, jnp.int32(v), jnp.int32(0))
    return out


def kernel(sizes, x_hbm, win_out, band_out, k_buf, j_buf, b_buf, k_stat, j_stat, b_stat,
           local_sem, k_recv, up_send, down_send, x_send, j_recv, j_send, b_recv, b_send, w_send, *band_wide):
    shard_count, windows, blocks, rows, width, jw, band, bw = sizes
    line = shard_count // COLS
    part_rows = rows // PARTS
    bits = blocks.bit_length() - 1
    chunks = shard_count * PARTS
    s = lax.axis_index("samp")
    n = lax.axis_index("snp")
    z = s // COLS
    x = s % COLS
    has_up = z < line - 1
    has_down = z > 0
    up = {"samp": jnp.minimum(s + COLS, shard_count - COLS + x)}
    down = {"samp": jnp.maximum(s - COLS, x)}
    across = {"samp": s + 1 - 2 * x}
    near = jnp.minimum(z, line - 1 - z)

    def bit(v, b):
        return (v // (1 << b)) % 2

    def flip(b):
        return {"snp": n + (1 << b) * (1 - 2 * bit(n, b))}

    j_home = (s * jw) // width
    j_off = pl.multiple_of((s * jw) % width, jw)
    b_home = (s * band) // width
    b_off = pl.multiple_of(((s * band) % width) // bw * bw, bw)
    j_rel = [(bit(n, b) + bit(j_home, b)) % 2 for b in range(bits)]
    b_rel = [(bit(n, b) + bit(b_home, b)) % 2 for b in range(bits)]

    def sends_on(rel, b):
        low = jnp.int32(0)
        for a in range(b + 1):
            low = low + rel[a]
        return low == 0

    def is_home(rel):
        total = jnp.int32(0)
        for r in rel:
            total = total + r
        return total == 0

    j_mine = is_home(j_rel)
    b_mine = is_home(b_rel)

    def k_copy(q, sem, to):
        return pltpu.make_async_remote_copy(
            src_ref=k_buf.at[q], dst_ref=k_buf.at[q], send_sem=sem.at[q], recv_sem=k_recv.at[q],
            device_id=to, device_id_type=MESH)

    def slice_copy(src, buf, q, send, recv, to):
        return pltpu.make_async_remote_copy(
            src_ref=src, dst_ref=buf.at[q], send_sem=send, recv_sem=recv.at[q],
            device_id=to, device_id_type=MESH)

    order = plan(line)
    band_sum = band_wide[0] if band_wide else band_out

    def item(o):
        side = lookup(o, [v[0] for v in order])
        r = lookup(o, [v[1] for v in order])
        c = lookup(o, [v[2] for v in order])
        odd = r % 2
        inner = z + jnp.where(odd == 1, 0 - (r + 1) // 2, r // 2)
        outer = jnp.where(z < line - 1 - z, r, line - 1 - r)
        zz = jnp.where(r <= 2 * near, inner, outer)
        xx = jnp.where(side == 1, 1 - x, x)
        return side, zz, c, (zz * COLS + xx) * PARTS + c

    def skips_x(zz, c):
        return (c == PARTS - 1) & ((zz == z + 1) | (zz == z - 1))

    for c in range(PARTS):
        pltpu.make_async_copy(x_hbm.at[pl.ds(c * part_rows, part_rows)],
                              k_buf.at[s * PARTS + c], local_sem.at[c]).start()

    barrier = pltpu.get_barrier_semaphore()

    def greet(to):
        pl.semaphore_signal(barrier, inc=1, device_id=to, device_id_type=MESH)

    pl.when(has_up)(lambda: greet(up))
    pl.when(has_down)(lambda: greet(down))
    greet(across)
    for b in range(bits):
        greet(flip(b))
    expected = 1 + bits
    if windows > 1:
        w = lax.axis_index("win")
        before = {"win": (w + windows - 1) % windows}
        after = {"win": (w + 1) % windows}
        greet(before)
        greet(after)
        expected += 2
    pl.semaphore_wait(barrier, expected + has_up.astype(jnp.int32) + has_down.astype(jnp.int32))

    k_stat[...] = jnp.zeros_like(k_stat)
    j_stat[...] = jnp.zeros_like(j_stat)
    b_stat[...] = jnp.zeros_like(b_stat)
    for c in range(PARTS):
        pltpu.make_async_copy(x_hbm.at[pl.ds(c * part_rows, part_rows)],
                              k_buf.at[s * PARTS + c], local_sem.at[c]).wait()

    last_own = max(i for i, v in enumerate(order) if v[0] == 0)
    cross_late = (s + 1 - 2 * x) * PARTS + PARTS - 1

    def take(o):
        side, zz, c, q = item(o)
        mine = (side == 0) & (zz == z)

        @pl.when(jnp.logical_not(mine))
        def _():
            k_copy(q, x_send, across).wait_recv()

        @pl.when((side == 0) & (zz <= z) & has_up)
        def _():
            k_copy(q, up_send, up).start()

        @pl.when((side == 0) & (zz >= z) & has_down)
        def _():
            k_copy(q, down_send, down).start()

        @pl.when((side == 0) & jnp.logical_not(skips_x(zz, c)))
        def _():
            k_copy(q, x_send, across).start()

        if line > 1:
            @pl.when((o == last_own) & has_up)
            def _():
                k_copy(cross_late, up_send, up).start()

            @pl.when((o == last_own) & has_down)
            def _():
                k_copy(cross_late, down_send, down).start()

        for b in reversed(range(bits)):
            @pl.when(j_mine)
            def _():
                slice_copy(k_buf.at[q, :, pl.ds(j_off, jw)], j_buf, q, j_send.at[b, q], j_recv, flip(b)).start()

            if windows == 1:
                @pl.when(b_mine)
                def _():
                    slice_copy(k_buf.at[q, :, pl.ds(b_off, bw)], b_buf, q, b_send.at[b, q], b_recv, flip(b)).start()
        if windows > 1:
            @pl.when(b_mine)
            def _():
                slice_copy(k_buf.at[q, :, pl.ds(b_off, bw)], b_buf, q, w_send.at[q], b_recv, before).start()

    def j_arrive(q):
        slice_copy(k_buf.at[q, :, pl.ds(j_off, jw)], j_buf, q, j_send.at[0, q], j_recv, flip(0)).wait_recv()

    def b_arrive(q):
        slice_copy(k_buf.at[q, :, pl.ds(b_off, bw)], b_buf, q, b_send.at[0, q], b_recv, flip(0)).wait_recv()

    def relay(o):
        _, _, _, q = item(o)

        @pl.when(jnp.logical_not(j_mine))
        def _():
            j_arrive(q)
            for b in reversed(range(bits)):
                @pl.when(sends_on(j_rel, b))
                def _():
                    slice_copy(j_buf.at[q], j_buf, q, j_send.at[b, q], j_recv, flip(b)).start()

        @pl.when(j_mine)
        def _():
            j_buf[q] = k_buf[q, :, pl.ds(j_off, jw)]

        def pass_band():
            b_arrive(q)
            for b in reversed(range(bits)):
                @pl.when(sends_on(b_rel, b))
                def _():
                    slice_copy(b_buf.at[q], b_buf, q, b_send.at[b, q], b_recv, flip(b)).start()

        if windows > 1:
            pass_band()
        else:
            pl.when(jnp.logical_not(b_mine))(pass_band)

            @pl.when(b_mine)
            def _():
                b_buf[q] = k_buf[q, :, pl.ds(b_off, bw)]

    def add_stats(stat, block):
        wide = block.astype(jnp.float32).reshape(part_rows // 8, 8, block.shape[-1])
        stat[0] += jnp.sum(wide, axis=0)
        stat[1] += jnp.sum(wide * wide, axis=0)

    def pair(a, b):
        return lax.dot_general(a, b, (((0,), (0,)), ((), ())), preferred_element_type=jnp.float32)

    def compute(o):
        _, _, _, q = item(o)
        whole = k_buf[q]
        j_cols = j_buf[q]
        b_cols = b_buf[q]
        add_stats(k_stat, whole)
        add_stats(j_stat, j_cols)
        add_stats(b_stat, b_cols)

        @pl.when(o == 0)
        def _():
            win_out[0] = pair(j_cols, whole)
            band_sum[0] = pair(b_cols, whole)

        @pl.when(o > 0)
        def _():
            win_out[0] += pair(j_cols, whole)
            band_sum[0] += pair(b_cols, whole)

    def step(o, carry):
        @pl.when(o < chunks)
        def _():
            take(o)

        @pl.when((o >= 2) & (o < chunks + 2))
        def _():
            relay(o - 2)

        @pl.when(o >= 3)
        def _():
            compute(o - 3)

        return carry

    lax.fori_loop(0, chunks + 3, step, 0)

    count = jnp.float32(rows * shard_count)

    def moments(total, square):
        mean = total / count
        return mean, 1.0 / jnp.maximum(square / count - mean * mean, VAR_FLOOR)

    row_mean, row_inv = moments(jnp.sum(k_stat[0], axis=0, keepdims=True), jnp.sum(k_stat[1], axis=0, keepdims=True))

    def finish(out, stat, height):
        mean, inv = moments(jnp.sum(stat[0].T, axis=1, keepdims=True), jnp.sum(stat[1].T, axis=1, keepdims=True))
        for a in range(0, height, 64):
            e = min(a + 64, height)
            covar = out[0, a:e] / count - mean[a:e] * row_mean
            out[0, a:e] = covar * covar * (inv[a:e] * row_inv)

    finish(win_out, j_stat, jw)
    finish(band_sum, b_stat, bw)
    if band_wide:
        band_out[0] = band_sum[0, pl.ds(pl.multiple_of((s * band) % bw, band), band)]

    def drain(o, carry):
        side, zz, c, q = item(o)

        @pl.when((side == 0) & (zz <= z) & has_up)
        def _():
            k_copy(q, up_send, up).wait_send()

        @pl.when((side == 0) & (zz >= z) & has_down)
        def _():
            k_copy(q, down_send, down).wait_send()

        @pl.when((side == 0) & jnp.logical_not(skips_x(zz, c)))
        def _():
            k_copy(q, x_send, across).wait_send()

        for b in range(bits):
            @pl.when(sends_on(j_rel, b))
            def _():
                slice_copy(j_buf.at[q], j_buf, q, j_send.at[b, q], j_recv, flip(b)).wait_send()

            @pl.when(sends_on(b_rel, b))
            def _():
                slice_copy(b_buf.at[q], b_buf, q, b_send.at[b, q], b_recv, flip(b)).wait_send()
        if windows > 1:
            @pl.when(b_mine)
            def _():
                slice_copy(b_buf.at[q], b_buf, q, w_send.at[q], b_recv, before).wait_send()
        return carry

    lax.fori_loop(0, chunks, drain, 0)
    if line > 1:
        @pl.when(has_up)
        def _():
            k_copy(cross_late, up_send, up).wait_send()

        @pl.when(has_down)
        def _():
            k_copy(cross_late, down_send, down).wait_send()


def shards(dosages):
    rows, width = dosages.shape
    shard_count = lax.axis_size("samp")
    windows = lax.axis_size("win")
    blocks = lax.axis_size("snp")
    jw = width * blocks // shard_count
    band = OV // shard_count
    bw = max(band, 128)
    bits = blocks.bit_length() - 1
    chunks = shard_count * PARTS
    part_rows = rows // PARTS
    sizes = (shard_count, windows, blocks, rows, width, jw, band, bw)
    dma = pltpu.SemaphoreType.DMA
    return pl.pallas_call(
        functools.partial(kernel, sizes),
        out_shape=(
            jax.ShapeDtypeStruct((1, jw, width), jnp.float32),
            jax.ShapeDtypeStruct((1, band, width), jnp.float32),
        ),
        in_specs=[pl.BlockSpec(memory_space=pl.ANY)],
        out_specs=[pl.BlockSpec(memory_space=pltpu.VMEM)] * 2,
        scratch_shapes=[
            pltpu.VMEM((chunks, part_rows, width), jnp.bfloat16),
            pltpu.VMEM((chunks, part_rows, jw), jnp.bfloat16),
            pltpu.VMEM((chunks, part_rows, bw), jnp.bfloat16),
            pltpu.VMEM((2, 8, width), jnp.float32),
            pltpu.VMEM((2, 8, jw), jnp.float32),
            pltpu.VMEM((2, 8, bw), jnp.float32),
            dma((PARTS,)),
            dma((chunks,)), dma((chunks,)), dma((chunks,)), dma((chunks,)),
            dma((chunks,)), dma((bits, chunks)),
            dma((chunks,)), dma((bits, chunks)), dma((chunks,)),
        ] + ([pltpu.VMEM((1, bw, width), jnp.float32)] if bw != band else []),
        compiler_params=pltpu.CompilerParams(
            collective_id=0, has_side_effects=True, vmem_limit_bytes=67043328
        ),
    )(dosages)


def solution(mesh):
    return jax.shard_map(
        shards,
        mesh=mesh,
        in_specs=(P("samp", ("win", "snp")),),
        out_specs=(P("win", "samp", "snp"), P("win", "samp", "snp")),
        check_vma=False,
    )
```

```python
import functools

import jax
import jax.numpy as jnp
from jax import lax
from jax.experimental import pallas as pl
from jax.experimental.pallas import tpu as pltpu
from jax.sharding import PartitionSpec as P

OV = 1024
VAR_FLOOR = 0.05
COLS = 2
PARTS = 2
MESH = pl.DeviceIdType.MESH


def plan(line):
    own = [(0, r, c) for r in range(line) for c in range(PARTS)]
    other = [(1, r, c) for r in range(line) for c in range(PARTS)]
    late = [v for v in other if v[1] in (1, 2) and v[2] == PARTS - 1]
    other = [v for v in other if v not in late]
    other = other[:-1] + [v for v in late if v[1] == 2] + other[-1:] + [v for v in late if v[1] == 1]
    lag = min(PARTS + 1, len(own))
    order = own[:lag]
    for k in range(lag, len(own)):
        order += [own[k], other[k - lag]]
    return order + other[len(own) - lag:]


def lookup(i, values):
    out = jnp.int32(0)
    for j, v in enumerate(values):
        if v:
            out = out + jnp.where(i == j, jnp.int32(v), jnp.int32(0))
    return out


def kernel(sizes, x_hbm, win_out, band_out, k_buf, j_buf, b_buf, k_stat, j_stat, b_stat,
           local_sem, k_recv, up_send, down_send, x_send, j_recv, j_send, b_recv, b_send, w_send, *band_wide):
    shard_count, windows, blocks, rows, width, jw, band, bw = sizes
    line = shard_count // COLS
    part_rows = rows // PARTS
    bits = blocks.bit_length() - 1
    chunks = shard_count * PARTS
    s = lax.axis_index("samp")
    n = lax.axis_index("snp")
    z = s // COLS
    x = s % COLS
    has_up = z < line - 1
    has_down = z > 0
    up = {"samp": jnp.minimum(s + COLS, shard_count - COLS + x)}
    down = {"samp": jnp.maximum(s - COLS, x)}
    across = {"samp": s + 1 - 2 * x}
    near = jnp.minimum(z, line - 1 - z)

    def bit(v, b):
        return (v // (1 << b)) % 2

    def flip(b):
        return {"snp": n + (1 << b) * (1 - 2 * bit(n, b))}

    j_home = (s * jw) // width
    j_off = pl.multiple_of((s * jw) % width, jw)
    b_home = (s * band) // width
    b_off = pl.multiple_of(((s * band) % width) // bw * bw, bw)
    j_rel = [(bit(n, b) + bit(j_home, b)) % 2 for b in range(bits)]
    b_rel = [(bit(n, b) + bit(b_home, b)) % 2 for b in range(bits)]

    def sends_on(rel, b):
        low = jnp.int32(0)
        for a in range(b + 1):
            low = low + rel[a]
        return low == 0

    def is_home(rel):
        total = jnp.int32(0)
        for r in rel:
            total = total + r
        return total == 0

    j_mine = is_home(j_rel)
    b_mine = is_home(b_rel)

    def k_copy(q, sem, to):
        return pltpu.make_async_remote_copy(
            src_ref=k_buf.at[q], dst_ref=k_buf.at[q], send_sem=sem.at[q], recv_sem=k_recv.at[q],
            device_id=to, device_id_type=MESH)

    def slice_copy(src, buf, q, send, recv, to):
        return pltpu.make_async_remote_copy(
            src_ref=src, dst_ref=buf.at[q], send_sem=send, recv_sem=recv.at[q],
            device_id=to, device_id_type=MESH)

    order = plan(line)
    band_sum = band_wide[0] if band_wide else band_out

    def item(o):
        side = lookup(o, [v[0] for v in order])
        r = lookup(o, [v[1] for v in order])
        c = lookup(o, [v[2] for v in order])
        odd = r % 2
        inner = z + jnp.where(odd == 1, 0 - (r + 1) // 2, r // 2)
        outer = jnp.where(z < line - 1 - z, r, line - 1 - r)
        zz = jnp.where(r <= 2 * near, inner, outer)
        xx = jnp.where(side == 1, 1 - x, x)
        return side, zz, c, (zz * COLS + xx) * PARTS + c

    def skips_x(zz, c):
        return (c == PARTS - 1) & ((zz == z + 1) | (zz == z - 1))

    for c in range(PARTS):
        pltpu.make_async_copy(x_hbm.at[pl.ds(c * part_rows, part_rows)],
                              k_buf.at[s * PARTS + c], local_sem.at[c]).start()

    barrier = pltpu.get_barrier_semaphore()

    def greet(to):
        pl.semaphore_signal(barrier, inc=1, device_id=to, device_id_type=MESH)

    pl.when(has_up)(lambda: greet(up))
    pl.when(has_down)(lambda: greet(down))
    greet(across)
    for b in range(bits):
        greet(flip(b))
    expected = 1 + bits
    if windows > 1:
        w = lax.axis_index("win")
        before = {"win": (w + windows - 1) % windows}
        after = {"win": (w + 1) % windows}
        greet(before)
        greet(after)
        expected += 2
    pl.semaphore_wait(barrier, expected + has_up.astype(jnp.int32) + has_down.astype(jnp.int32))

    k_stat[...] = jnp.zeros_like(k_stat)
    j_stat[...] = jnp.zeros_like(j_stat)
    b_stat[...] = jnp.zeros_like(b_stat)
    for c in range(PARTS):
        pltpu.make_async_copy(x_hbm.at[pl.ds(c * part_rows, part_rows)],
                              k_buf.at[s * PARTS + c], local_sem.at[c]).wait()

    last_own = max(i for i, v in enumerate(order) if v[0] == 0)
    cross_late = (s + 1 - 2 * x) * PARTS + PARTS - 1

    def take(o):
        side, zz, c, q = item(o)
        mine = (side == 0) & (zz == z)

        @pl.when(jnp.logical_not(mine))
        def _():
            k_copy(q, x_send, across).wait_recv()

        @pl.when((side == 0) & (zz <= z) & has_up)
        def _():
            k_copy(q, up_send, up).start()

        @pl.when((side == 0) & (zz >= z) & has_down)
        def _():
            k_copy(q, down_send, down).start()

        @pl.when((side == 0) & jnp.logical_not(skips_x(zz, c)))
        def _():
            k_copy(q, x_send, across).start()

        if line > 1:
            @pl.when((o == last_own) & has_up)
            def _():
                k_copy(cross_late, up_send, up).start()

            @pl.when((o == last_own) & has_down)
            def _():
                k_copy(cross_late, down_send, down).start()

        for b in reversed(range(bits)):
            @pl.when(j_mine)
            def _():
                slice_copy(k_buf.at[q, :, pl.ds(j_off, jw)], j_buf, q, j_send.at[b, q], j_recv, flip(b)).start()

            if windows == 1:
                @pl.when(b_mine)
                def _():
                    slice_copy(k_buf.at[q, :, pl.ds(b_off, bw)], b_buf, q, b_send.at[b, q], b_recv, flip(b)).start()
        if windows > 1:
            @pl.when(b_mine)
            def _():
                slice_copy(k_buf.at[q, :, pl.ds(b_off, bw)], b_buf, q, w_send.at[q], b_recv, before).start()

    def j_arrive(q):
        slice_copy(k_buf.at[q, :, pl.ds(j_off, jw)], j_buf, q, j_send.at[0, q], j_recv, flip(0)).wait_recv()

    def b_arrive(q):
        slice_copy(k_buf.at[q, :, pl.ds(b_off, bw)], b_buf, q, b_send.at[0, q], b_recv, flip(0)).wait_recv()

    def relay(o):
        _, _, _, q = item(o)

        @pl.when(jnp.logical_not(j_mine))
        def _():
            j_arrive(q)
            for b in reversed(range(bits)):
                @pl.when(sends_on(j_rel, b))
                def _():
                    slice_copy(j_buf.at[q], j_buf, q, j_send.at[b, q], j_recv, flip(b)).start()

        @pl.when(j_mine)
        def _():
            j_buf[q] = k_buf[q, :, pl.ds(j_off, jw)]

        def pass_band():
            b_arrive(q)
            for b in reversed(range(bits)):
                @pl.when(sends_on(b_rel, b))
                def _():
                    slice_copy(b_buf.at[q], b_buf, q, b_send.at[b, q], b_recv, flip(b)).start()

        if windows > 1:
            pass_band()
        else:
            pl.when(jnp.logical_not(b_mine))(pass_band)

            @pl.when(b_mine)
            def _():
                b_buf[q] = k_buf[q, :, pl.ds(b_off, bw)]

    def add_stats(stat, block):
        wide = block.astype(jnp.float32).reshape(part_rows // 8, 8, block.shape[-1])
        stat[0] += jnp.sum(wide, axis=0)
        stat[1] += jnp.sum(wide * wide, axis=0)

    def pair(a, b):
        return lax.dot_general(a, b, (((0,), (0,)), ((), ())), preferred_element_type=jnp.float32)

    def compute(o):
        _, _, _, q = item(o)
        whole = k_buf[q]
        j_cols = j_buf[q]
        b_cols = b_buf[q]
        add_stats(k_stat, whole)
        add_stats(j_stat, j_cols)
        add_stats(b_stat, b_cols)

        @pl.when(o == 0)
        def _():
            win_out[0] = pair(j_cols, whole)
            band_sum[0] = pair(b_cols, whole)

        @pl.when(o > 0)
        def _():
            win_out[0] += pair(j_cols, whole)
            band_sum[0] += pair(b_cols, whole)

    def step(o, carry):
        @pl.when(o < chunks)
        def _():
            take(o)

        @pl.when((o >= 3) & (o < chunks + 3))
        def _():
            relay(o - 3)

        @pl.when(o >= 4)
        def _():
            compute(o - 4)

        return carry

    lax.fori_loop(0, chunks + 4, step, 0)

    count = jnp.float32(rows * shard_count)

    def moments(total, square):
        mean = total / count
        return mean, 1.0 / jnp.maximum(square / count - mean * mean, VAR_FLOOR)

    row_mean, row_inv = moments(jnp.sum(k_stat[0], axis=0, keepdims=True), jnp.sum(k_stat[1], axis=0, keepdims=True))

    def finish(out, stat, height):
        mean, inv = moments(jnp.sum(stat[0].T, axis=1, keepdims=True), jnp.sum(stat[1].T, axis=1, keepdims=True))
        for a in range(0, height, 64):
            e = min(a + 64, height)
            covar = out[0, a:e] / count - mean[a:e] * row_mean
            out[0, a:e] = covar * covar * (inv[a:e] * row_inv)

    finish(win_out, j_stat, jw)
    finish(band_sum, b_stat, bw)
    if band_wide:
        band_out[0] = band_sum[0, pl.ds(pl.multiple_of((s * band) % bw, band), band)]

    def drain(o, carry):
        side, zz, c, q = item(o)

        @pl.when((side == 0) & (zz <= z) & has_up)
        def _():
            k_copy(q, up_send, up).wait_send()

        @pl.when((side == 0) & (zz >= z) & has_down)
        def _():
            k_copy(q, down_send, down).wait_send()

        @pl.when((side == 0) & jnp.logical_not(skips_x(zz, c)))
        def _():
            k_copy(q, x_send, across).wait_send()

        for b in range(bits):
            @pl.when(sends_on(j_rel, b))
            def _():
                slice_copy(j_buf.at[q], j_buf, q, j_send.at[b, q], j_recv, flip(b)).wait_send()

            @pl.when(sends_on(b_rel, b))
            def _():
                slice_copy(b_buf.at[q], b_buf, q, b_send.at[b, q], b_recv, flip(b)).wait_send()
        if windows > 1:
            @pl.when(b_mine)
            def _():
                slice_copy(b_buf.at[q], b_buf, q, w_send.at[q], b_recv, before).wait_send()
        return carry

    lax.fori_loop(0, chunks, drain, 0)
    if line > 1:
        @pl.when(has_up)
        def _():
            k_copy(cross_late, up_send, up).wait_send()

        @pl.when(has_down)
        def _():
            k_copy(cross_late, down_send, down).wait_send()


def shards(dosages):
    rows, width = dosages.shape
    shard_count = lax.axis_size("samp")
    windows = lax.axis_size("win")
    blocks = lax.axis_size("snp")
    jw = width * blocks // shard_count
    band = OV // shard_count
    bw = max(band, 128)
    bits = blocks.bit_length() - 1
    chunks = shard_count * PARTS
    part_rows = rows // PARTS
    sizes = (shard_count, windows, blocks, rows, width, jw, band, bw)
    dma = pltpu.SemaphoreType.DMA
    return pl.pallas_call(
        functools.partial(kernel, sizes),
        out_shape=(
            jax.ShapeDtypeStruct((1, jw, width), jnp.float32),
            jax.ShapeDtypeStruct((1, band, width), jnp.float32),
        ),
        in_specs=[pl.BlockSpec(memory_space=pl.ANY)],
        out_specs=[pl.BlockSpec(memory_space=pltpu.VMEM)] * 2,
        scratch_shapes=[
            pltpu.VMEM((chunks, part_rows, width), jnp.bfloat16),
            pltpu.VMEM((chunks, part_rows, jw), jnp.bfloat16),
            pltpu.VMEM((chunks, part_rows, bw), jnp.bfloat16),
            pltpu.VMEM((2, 8, width), jnp.float32),
            pltpu.VMEM((2, 8, jw), jnp.float32),
            pltpu.VMEM((2, 8, bw), jnp.float32),
            dma((PARTS,)),
            dma((chunks,)), dma((chunks,)), dma((chunks,)), dma((chunks,)),
            dma((chunks,)), dma((bits, chunks)),
            dma((chunks,)), dma((bits, chunks)), dma((chunks,)),
        ] + ([pltpu.VMEM((1, bw, width), jnp.float32)] if bw != band else []),
        compiler_params=pltpu.CompilerParams(
            collective_id=0, has_side_effects=True, vmem_limit_bytes=67043328
        ),
    )(dosages)


def solution(mesh):
    return jax.shard_map(
        shards,
        mesh=mesh,
        in_specs=(P("samp", ("win", "snp")),),
        out_specs=(P("win", "samp", "snp"), P("win", "samp", "snp")),
        check_vma=False,
    )
```
